256 devices in a mesh: leaf: 256 (over x, z, y, core).
Axes of the slice: x: 4, y: 4, z: 8, core: 2. Of those that a mesh axis runs over, the one named last changes fastest.
Arguments:
- random_block: bfloat16 [131072, 256], P('leaf'), may hold values from -6 to 6
- diag_block: bfloat16 [131072, 512], P('leaf'), may hold values from -0.25 to 0.25
- basis_out: bfloat16 [131072, 256], P('leaf'), may hold values from -0.1875 to 0.1875
- basis_in: bfloat16 [131072, 256], P('leaf'), may hold values from -0.25 to 0.25
- low_up: bfloat16 [256, 5, 256, 256], P('leaf'), as said below
- low_down: bfloat16 [256, 5, 256, 256], P('leaf'), as said below
- low_coupling: bfloat16 [256, 5, 256, 256], P('leaf'), as said below
- top_up: bfloat16 [12, 256, 256], replicated, may hold values from -0.25 to 0.25
- top_down: bfloat16 [12, 256, 256], replicated, may hold values from -0.375 to 0.375
- top_coupling: bfloat16 [14, 256, 256], replicated, may hold values from -0.375 to 0.375
Outputs:
- sample: bfloat16 [131072, 256], P('leaf')
The draws below stay inside these ranges and needn't reach their ends.
Inputs may be any that keep to these rules, and one draw needn't show every extreme that they name: `low_up`: for every level l below 5, entries [i, l] and [j, l] are the same matrix when i // 2^l == j // 2^l. `low_down`: for every level l below 5, entries [i, l] and [j, l] are the same matrix when i // 2^l == j // 2^l. `low_coupling`: for every level l below 5, entries [i, l] and [j, l] are the same matrix when i // 2^l == j // 2^l.
All inputs are finite; a program needn't handle non-finite values.
Results may differ from the reference program's by a relative error of at most 0.018.
Values may be sent and summed in bfloat16 or wider, within the bound.
A program may use at most 64 MiB of HBM per device.

```python
import jax
import jax.numpy as jnp

LEAF = 512
RANK = 256
NCOL = 256
TOP = 3
LOW = 5
ORDER = 131072
TOPNODES = 14
TOPINNER = 12
N_LEAF = 256


def replicated_levels(key, scale):
    leaves = ORDER // LEAF
    stacked = []
    for height in range(LOW):
        node_count = leaves // 2 ** height
        subkey = jax.random.fold_in(key, height)
        values = jax.random.normal(subkey, (node_count, RANK, RANK), jnp.float32) * scale
        stacked.append(jnp.repeat(values, 2 ** height, axis=0))
    return jnp.stack(stacked, axis=1).astype(jnp.bfloat16)


def draw_low_up(key, part):
    return replicated_levels(jax.random.fold_in(key, 101), (2.0 * RANK) ** (-0.5))


def draw_low_down(key, part):
    return replicated_levels(jax.random.fold_in(key, 202), RANK ** (-0.5))


def draw_low_coupling(key, part):
    return replicated_levels(jax.random.fold_in(key, 303), RANK ** (-0.5))


def levels(stream_key, shape, shards, low, top_value):
    def one(position, blocks):
        draws = jax.random.uniform(jax.random.fold_in(jax.random.fold_in(stream_key, 6), position), (blocks,), jnp.float32, low / len(shards), top_value / len(shards))
        return jnp.repeat(jnp.exp(draws), shape[position] // blocks).reshape((-1,) + (1,) * (len(shape) - position - 1))

    level = one(*shards[0])
    for cut in shards[1:]:
        level = level * one(*cut)
    return level


def normal_values(stream_key, dims, scale, reach, pieces=(), kind=jnp.bfloat16):
    drawn = jax.random.normal(stream_key, dims, jnp.float32) * scale
    if len(pieces) > 0:
        drawn = levels(stream_key, dims, pieces, -0.22, 0.18) * drawn
    return jnp.clip(drawn, min=-reach, max=reach).astype(kind)


def setup_inputs(seed: int = 0) -> dict:
    streams_of = jax.random.split(jax.random.key(seed), 11)
    random_block = normal_values(streams_of[0], (ORDER, NCOL), 1.0, 6.0, ((0, 256),))
    diag_block = normal_values(streams_of[1], (ORDER, LEAF), LEAF ** -0.5, 0.25, ((0, 256),))
    basis_out = normal_values(streams_of[2], (ORDER, RANK), (4 * RANK) ** -0.5, 0.1875, ((0, 256),))
    basis_in = normal_values(streams_of[3], (ORDER, RANK), LEAF ** -0.5, 0.25, ((0, 256),))
    low_up = draw_low_up(jax.random.fold_in(streams_of[10], 71), 0)
    low_down = draw_low_down(jax.random.fold_in(streams_of[10], 71), 0)
    low_coupling = draw_low_coupling(jax.random.fold_in(streams_of[10], 71), 0)
    top_up = normal_values(streams_of[7], (TOPINNER, RANK, RANK), (2 * RANK) ** -0.5, 0.25)
    top_down = normal_values(streams_of[8], (TOPINNER, RANK, RANK), RANK ** -0.5, 0.375)
    top_coupling = normal_values(streams_of[9], (TOPNODES, RANK, RANK), RANK ** -0.5, 0.375)
    return {"random_block": random_block, "diag_block": diag_block, "basis_out": basis_out, "basis_in": basis_in, "low_up": low_up, "low_down": low_down, "low_coupling": low_coupling, "top_up": top_up, "top_down": top_down, "top_coupling": top_coupling}


def level_generators(lower, upper, height, low_levels):
    if height < low_levels:
        return lower[:: 2 ** height, height]
    section = height - low_levels
    offset = 2 ** (TOP + 1) - 2 ** (TOP + 1 - section)
    node_count = 2 ** (TOP - section)
    return upper[offset:offset + node_count]


def batch_trans(matrix, values):
    return jnp.einsum("nrs,nrc->nsc", matrix.astype(jnp.float32), values.astype(jnp.float32))


def batch_apply(matrix, values):
    return jnp.einsum("nrs,nsc->nrc", matrix.astype(jnp.float32), values.astype(jnp.float32))


def reference(random_block, diag_block, basis_out, basis_in, low_up, low_down, low_coupling, top_up, top_down, top_coupling):
    levels_total = N_LEAF.bit_length() - 1
    low_levels = levels_total - TOP
    leaf_cols = random_block.reshape(N_LEAF, LEAF, NCOL)
    current = batch_trans(basis_in.reshape(N_LEAF, LEAF, RANK), leaf_cols)
    couplings = []
    for height in range(levels_total):
        node_count = current.shape[0]
        rounded = current.astype(jnp.bfloat16)
        swapped = rounded.reshape(node_count // 2, 2, RANK, NCOL)[:, ::-1].reshape(node_count, RANK, NCOL)
        coupler = level_generators(low_coupling, top_coupling, height, low_levels)
        couplings.append(batch_apply(coupler, swapped))
        if height < levels_total - 1:
            lifter = level_generators(low_up, top_up, height, low_levels)
            lifted = batch_trans(lifter, rounded).astype(jnp.bfloat16).astype(jnp.float32)
            paired = lifted.reshape(node_count // 2, 2, RANK, NCOL)
            current = paired[:, 0] + paired[:, 1]
    descent = couplings[-1]
    for height in range(levels_total - 2, -1, -1):
        parent = jnp.repeat(descent.astype(jnp.bfloat16), 2, axis=0)
        lowering = level_generators(low_down, top_down, height, low_levels)
        descent = batch_apply(lowering, parent) + couplings[height]
    local = batch_apply(diag_block.reshape(N_LEAF, LEAF, LEAF), leaf_cols)
    spread = batch_apply(basis_out.reshape(N_LEAF, LEAF, RANK), descent.astype(jnp.bfloat16))
    return (local + spread).reshape(ORDER, NCOL).astype(jnp.bfloat16)
```

```python
import jax
import jax.numpy as jnp
from jax import lax
from jax.experimental import pallas as pl
from jax.experimental.pallas import tpu as pltpu
from jax.sharding import PartitionSpec as P

BF = jnp.bfloat16
F32 = jnp.float32
ROWS = 32


def mm(a, b):
    return jnp.dot(a, b, preferred_element_type=F32)


def mmt(a, b):
    return lax.dot_general(a, b, (((1,), (1,)), ((), ())), preferred_element_type=F32)


def body(
    x_h, d_h, u_h, v_h, lw_h, lr_h, lb_h, tw_h, tr_h, tb_h,
    out,
    x_v, d_v, u_v, v_v, w_v, r_v, b_v, tw_v, tr_v, tb_v,
    c0, c0s, p1, p1r, p3, yrecv, c3, p4, p4r, c3r, zrecv, xrecv,
    c1h, p2h, p2r, c2h, c1s, c2s, zall, base, k5, k6, ka, kb, ur,
    load_sem, send_sem, recv_sem,
):
    me = lax.axis_index("leaf")
    core = me % 2
    y = (me // 2) % 4
    z = (me // 8) % 8
    x = me // 64
    p = me % 8
    zl = z % 4
    zh = z // 4

    def dev(xx, zz, yy, cc):
        return ((xx * 8 + zz) * 4 + yy) * 2 + cc

    y_peers = [
        (dev(x, z, (y + dy) % 4, (core + dc) % 2), ((y + dy) % 4) * 2 + (core + dc) % 2)
        for dy, dc in ((2, 0), (2, 1), (1, 0), (3, 0), (1, 1), (3, 1), (0, 1))
    ]
    y_from = [
        ((y - dy + 4) % 4) * 2 + (core + dc) % 2
        for dy, dc in ((2, 0), (2, 1), (1, 0), (3, 0), (1, 1), (3, 1), (0, 1))
    ]
    z_peers = [dev(x, (z + dz) % 8, y, core) for dz in (4, 3, 5, 2, 6, 1, 7)]
    x_peers = [dev((x + dx) % 4, z, y, core) for dx in (2, 1, 3)]
    mate = dev(x, z, y, 1 - core)
    y1 = dev(x, z, y + 1 - 2 * (y % 2), core)
    y2 = dev(x, z, (y + 2) % 4, core)

    barrier = pltpu.get_barrier_semaphore()
    peers = [q[0] for q in y_peers] + z_peers + x_peers
    for peer in peers:
        pl.semaphore_signal(barrier, inc=1, device_id=(peer,), device_id_type=pl.DeviceIdType.MESH)

    loads = {}

    def load(name, src, dst):
        k = len(loads)
        loads[name] = pltpu.make_async_copy(src, dst, load_sem.at[k])
        loads[name].start()

    n5, n6, n7 = me // 32, me // 64, me // 128
    load("x", x_h, x_v)
    load("v", v_h, v_v)
    for l in range(3):
        load(f"w{l}", lw_h.at[0, l], w_v.at[l])
    for l in range(3, 5):
        load(f"w{l}", lw_h.at[0, l], w_v.at[l])
    sib5 = n5 + 1 - 2 * (n5 % 2)
    far = (1 - n7) * 2
    load("w5o", tw_h.at[n5], tw_v.at[0])
    load("w5s", tw_h.at[sib5], tw_v.at[1])
    load("w6a", tw_h.at[8 + far], tw_v.at[2])
    load("w6b", tw_h.at[8 + far + 1], tw_v.at[3])
    load("r5", tr_h.at[n5], tr_v.at[0])
    load("r6", tr_h.at[8 + n6], tr_v.at[1])
    load("b5", tb_h.at[n5], tb_v.at[0])
    load("b6", tb_h.at[8 + n6], tb_v.at[1])
    load("b7", tb_h.at[12 + n7], tb_v.at[2])
    load("r", lr_h.at[0], r_v)
    load("b", lb_h.at[0], b_v)
    load("u", u_h, u_v)
    load("d", d_h, d_v)

    sent = []

    def copy(src, dst, k, peer):
        return pltpu.make_async_remote_copy(
            src_ref=src, dst_ref=dst, send_sem=send_sem.at[k], recv_sem=recv_sem.at[k],
            device_id=(peer,), device_id_type=pl.DeviceIdType.MESH,
        )

    def send(src, dst, k, peer):
        c = copy(src, dst, k, peer)
        c.start()
        sent.append(c)
        return c

    loads["x"].wait()
    loads["v"].wait()
    c0[...] = lax.dot_general(
        x_v[...], v_v[...], (((0,), (0,)), ((), ())), preferred_element_type=F32
    ).astype(BF)
    loads["w0"].wait()
    p1[...] = mm(c0[...], w_v[0]).astype(BF).reshape(2, 128, 256)
    loads["w1"].wait()
    p2 = mm(p1[...].reshape(256, 256), w_v[1]).astype(BF)
    loads["w2"].wait()
    p3[...] = mm(p2, w_v[2]).astype(BF).reshape(8, ROWS, 256)

    pl.semaphore_wait(barrier, len(peers))

    y_up = [send(p3.at[q], yrecv.at[i], i, peer) for i, (peer, q) in enumerate(y_peers)]
    m_c0 = send(c0, c0s, 7, mate)
    m_p1 = send(p1.at[1 - core], p1r, 8, mate)

    for n in ("w3", "w4", "w5o", "w5s", "w6a", "w6b", "r5", "r6", "b5", "b6", "b7", "r", "b"):
        loads[n].wait()
    r4 = r_v[4]
    r5 = tr_v[0]
    k5[...] = mm(r4, tb_v[0]).astype(BF)
    t = mm(r5, tb_v[1]).astype(BF)
    k6[...] = mm(r4, t).astype(BF)
    t = mm(tr_v[1], tb_v[2]).astype(BF)
    t = mm(r5, t).astype(BF)
    t = mm(r4, t).astype(BF)
    ka[...] = mmt(t, tw_v[2]).astype(BF)
    kb[...] = mmt(t, tw_v[3]).astype(BF)

    m_p1.wait_recv()
    half = (p1[core].astype(F32) + p1r[...].astype(F32)).astype(BF)
    c1h[...] = half
    p2h[...] = mm(half, w_v[1]).astype(BF)

    for c in y_up:
        c.wait_recv()
    total = p3[p].astype(F32)
    for i in range(7):
        total += yrecv[i].astype(F32)
    c3v = total.astype(BF)
    c3[...] = c3v
    p4v = mm(c3v, w_v[3]).astype(BF)
    p4[...] = p4v
    zrecv[z] = mm(p4v, w_v[4]).astype(BF)

    z_up = [send(zrecv.at[z], zrecv.at[z], 9 + i, peer) for i, peer in enumerate(z_peers)]
    cousin = zh * 4 + (1 - zl // 2) * 2
    s4 = [
        send(p4, p4r.at[zl % 2], 16 + i, dev(x, cousin + (zl + i) % 2, y, core)) for i in range(2)
    ]
    s3 = send(c3, c3r, 18, dev(x, z + 1 - 2 * (z % 2), y, core))
    s_c1 = send(c1h, c1s.at[core], 19, y1)
    s_p2 = send(p2h, p2r, 20, y1)

    loads["u"].wait()
    loads["d"].wait()
    base[...] = mm(d_v[...], x_v[...])
    ur[...] = mm(u_v[...], r_v[0]).astype(BF)
    m_c0.wait_recv()
    f0 = mmt(c0s[...], b_v[0]).astype(BF)
    base[...] += mmt(u_v[...], f0)

    s_p2.wait_recv()
    c2h[...] = (p2h[...].astype(F32) + p2r[...].astype(F32)).astype(BF)
    s_c2 = send(c2h, c2s.at[core], 21, y2)
    s_c1.wait_recv()
    m_c1 = send(c1s.at[core], c1s.at[core], 22, mate)

    for c in z_up:
        c.wait_recv()
    own = zrecv[zh * 4].astype(F32)
    sib = zrecv[(1 - zh) * 4].astype(F32)
    for j in range(1, 4):
        own += zrecv[zh * 4 + j].astype(F32)
        sib += zrecv[(1 - zh) * 4 + j].astype(F32)
    c5o = own.astype(BF)
    c5s = sib.astype(BF)
    xrecv[x] = (mm(c5o, tw_v[0]) + mm(c5s, tw_v[1])).astype(BF)
    x_up = [send(xrecv.at[x], xrecv.at[x], 23 + i, peer) for i, peer in enumerate(x_peers)]

    for c in s4:
        c.wait_recv()
    c4s = (p4r[0].astype(F32) + p4r[1].astype(F32)).astype(BF)
    pre4 = mmt(c5s, k5[...]) + mmt(c4s, b_v[4])
    s3.wait_recv()
    f3 = mmt(c3r[...], b_v[3])

    for c in x_up:
        c.wait_recv()
    near = x + 1 - 2 * (x % 2)
    xfar = (1 - x // 2) * 2
    v4 = pre4 + mmt(xrecv[near], k6[...]) + mmt(xrecv[xfar], ka[...]) + mmt(xrecv[xfar + 1], kb[...])
    zall[p] = (mmt(v4.astype(BF), r_v[3]) + f3).astype(BF)
    z_dn = [send(zall.at[p], zall.at[p], 26 + i, peer) for i, (peer, q) in enumerate(y_peers)]

    s_c2.wait_recv()
    m_c2 = send(c2s.at[core], c2s.at[core], 33, mate)
    m_c1.wait_recv()
    f1 = mmt(c1s[...].reshape(256, 256), b_v[1])
    m_c2.wait_recv()
    f2 = mmt(c2s[...].reshape(256, 256), b_v[2])

    for c in z_dn:
        c.wait_recv()
    z3 = zall[...].reshape(256, 256)
    z2 = (mmt(z3, r_v[2]) + f2).astype(BF)
    z1 = (mmt(z2, r_v[1]) + f1).astype(BF)
    out[...] = (base[...] + mmt(ur[...], z1)).astype(BF)

    for c in sent:
        c.wait_send()


def per_device(*args):
    any_spec = pl.BlockSpec(memory_space=pltpu.HBM)
    sq = (256, 256)
    vm = lambda *s: pltpu.VMEM(s, BF)
    return pl.pallas_call(
        body,
        out_shape=jax.ShapeDtypeStruct((512, 256), BF),
        in_specs=[any_spec] * 10,
        out_specs=pl.BlockSpec(memory_space=pltpu.VMEM),
        scratch_shapes=[
            vm(512, 256), vm(512, 512), vm(512, 256), vm(512, 256),
            vm(5, *sq), vm(5, *sq), vm(5, *sq), vm(4, *sq), vm(2, *sq), vm(3, *sq),
            vm(*sq), vm(*sq), vm(2, 128, 256), vm(128, 256), vm(8, ROWS, 256), vm(7, ROWS, 256),
            vm(ROWS, 256), vm(ROWS, 256), vm(2, ROWS, 256), vm(ROWS, 256), vm(8, ROWS, 256),
            vm(4, ROWS, 256),
            vm(128, 256), vm(128, 256), vm(128, 256), vm(128, 256), vm(2, 128, 256), vm(2, 128, 256),
            vm(8, ROWS, 256), pltpu.VMEM((512, 256), F32),
            vm(*sq), vm(*sq), vm(*sq), vm(*sq), vm(512, 256),
            pltpu.SemaphoreType.DMA((24,)),
            pltpu.SemaphoreType.DMA((34,)),
            pltpu.SemaphoreType.DMA((34,)),
        ],
        compiler_params=pltpu.CompilerParams(
            collective_id=0, has_side_effects=True, vmem_limit_bytes=66000000
        ),
        name="hss",
    )(*args)


def solution(mesh):
    placed = (
        P("leaf", None),
        P("leaf", None),
        P("leaf", None),
        P("leaf", None),
        P("leaf", None, None, None),
        P("leaf", None, None, None),
        P("leaf", None, None, None),
        P(),
        P(),
        P(),
    )
    return jax.shard_map(
        per_device, mesh=mesh, in_specs=placed, out_specs=P("leaf", None), check_vma=False
    )
```
